32 devices in a mesh: groups: 2 (over x), ctx: 16 (over z, y, core).
Axes of the slice: x: 2, y: 2, z: 4, core: 2. Of those that a mesh axis runs over, the one named last changes fastest.
Arguments:
- queries: bfloat16 [512, 128, 576], P(('groups', 'ctx')), parts along dimension 0, may hold values from -4 to 4
- latent_cache: bfloat16 [32768, 576], P(('groups', 'ctx')), parts along dimension 0, may hold values from -4 to 4
- block_picks: int32 [32, 32], P(('groups', 'ctx')), parts along dimension 0, may hold values from 0 to 255, as said below
- lengths: int32 [512], P(('groups', 'ctx')), parts along dimension 0, may hold values from 8192 to 16384
Outputs:
- latent_out: bfloat16 [512, 128, 512], P(('groups', 'ctx')), parts along dimension 0
The draws below stay inside these ranges and needn't reach their ends.
There are 2 independent parts, one for each index of `groups`. The reference program is written for one: setup_inputs(seed, part) draws one part's arguments, and reference() takes and returns one part's arrays. A program takes and returns all parts, laid end to end along the dimension named above; each array names one. Nothing has to cross between parts.
Inputs may be any that keep to these rules, and one draw needn't show every extreme that they name: `block_picks`: each row names 32 different blocks. At most 4 of a row's blocks lie in one owner's range of 16 consecutive blocks, and every row reaches this with its first 4 entries, which lie in the first half of the context. Over all rows together at most 8 different blocks of one owner's range are named, and some owner reaches this.
All inputs are finite; a program needn't handle non-finite values.
Results may differ from the reference program's by a relative error of at most 0.0035.
Values may be sent and summed in bfloat16 or wider, within the bound.
No kernel may reach another device: no remote copies, remote signals or barrier semaphores. Data moves between devices by JAX's collectives and lax.ppermute only.
A program may use at most 128 MiB of HBM per device.

```python
import jax
import jax.numpy as jnp
from jax import lax

H = 128
LAT = 512
BLOCK = 64
TOPK = 32
BLK_DEV = 16
WIDTH = 576
CONTEXT = 16384
QROWS = 256
N_CTX = 16


def draw_latent_cache(key, part):
    seed_cache = jax.random.fold_in(key, 21)
    values = jnp.clip(jax.random.normal(seed_cache, (CONTEXT, WIDTH), jnp.float32), -4.0, 4.0)
    return values.astype(jnp.bfloat16)


def draw_block_picks(key, part):
    capacity = max(1, 2 * TOPK // N_CTX)
    pair_count = N_CTX * capacity
    starting_picks = jax.random.fold_in(key, 41)
    popular_region_seed, extra_credit_seed, noise_perturbation_seed, permutation_seed, split_choice_seed = jax.random.split(starting_picks, 5)
    hot_owner = jax.random.randint(popular_region_seed, (N_CTX,), 0, max(1, N_CTX // 2))
    hot_owner = hot_owner.at[1].set(hot_owner[0])
    owner_preference_lift = jax.random.randint(extra_credit_seed, (N_CTX,), 0, 2) * 4096
    jitter_amount = jax.random.randint(noise_perturbation_seed, (N_CTX, pair_count), 0, 4096)
    pair_index = jnp.arange(pair_count, dtype=jnp.int32)
    every_pair_holder = pair_index // capacity
    required_blocks = (every_pair_holder[None, :] == hot_owner[:, None]).astype(jnp.int32) * 16384
    block_ratings = jitter_amount + owner_preference_lift[every_pair_holder][None, :] + required_blocks
    block_ratings = block_ratings * pair_count + pair_index[None, :]
    _, chosen = lax.top_k(block_ratings, TOPK)
    pair_owner = chosen // capacity
    pair_slot = chosen % capacity
    ranks = jax.random.randint(permutation_seed, (N_CTX, BLK_DEV), 0, 65536) * BLK_DEV + jnp.arange(BLK_DEV, dtype=jnp.int32)[None, :]
    candidates = jnp.argsort(ranks, axis=1)[:, :2 * capacity].astype(jnp.int32)
    side_bit = jax.random.randint(split_choice_seed, (N_CTX, TOPK), 0, 2)
    group_index = jnp.arange(N_CTX, dtype=jnp.int32)[:, None]
    at_shared = pair_owner == hot_owner[0]
    side_bit = jnp.where((group_index == 0) & at_shared, 0, side_bit)
    side_bit = jnp.where((group_index == 1) & at_shared, 1, side_bit)
    local_block = candidates[pair_owner, 2 * pair_slot + side_bit]
    return (pair_owner * BLK_DEV + local_block).astype(jnp.int32)


def draw_queries(key, part):
    seed_rows = jax.random.fold_in(key, 31)
    array_shape = (QROWS, H, WIDTH)
    values = jnp.clip(jax.random.normal(seed_rows, array_shape, jnp.float32), -4.0, 4.0)
    return values.astype(jnp.bfloat16)


def plant(values, key, least, top_value):
    extent = values.shape
    spot = [jax.random.randint(jax.random.fold_in(key, axis), (), 0, extent[axis]) for axis in range(len(extent))]
    values = values.at[tuple(spot)].set(least)
    longest = extent.index(max(extent))
    spot[longest] = (spot[longest] + 1) % extent[longest]
    return values.at[tuple(spot)].set(top_value)


def setup_inputs(seed: int = 0, part: int = 0) -> dict:
    key_of = jax.random.split(jax.random.key(seed), 5)
    part_keys = jax.random.split(jax.random.fold_in(key_of[4], part), 5)
    queries = draw_queries(jax.random.fold_in(jax.random.fold_in(key_of[4], part), 71), part)
    latent_cache = draw_latent_cache(jax.random.fold_in(jax.random.fold_in(key_of[4], part), 71), part)
    block_picks = draw_block_picks(jax.random.fold_in(jax.random.fold_in(key_of[4], part), 71), part)
    lengths = plant(jax.random.randint(part_keys[3], (QROWS,), CONTEXT // 2, CONTEXT + 1), jax.random.fold_in(part_keys[3], 1), CONTEXT // 2, CONTEXT).astype(jnp.int32)
    return dict(queries=queries, latent_cache=latent_cache, block_picks=block_picks, lengths=lengths)


SOFTMAX_SCALE = 192.0 ** -0.5


def attend(query_rows, key_rows, positions, row_lengths):
    total_rows = query_rows.shape[0]
    step_rows = 512 if total_rows % 512 == 0 else total_rows
    block_count = total_rows // step_rows
    latent = key_rows[:, :LAT]

    def per_block(inputs):
        block_queries, block_lengths = inputs
        block_ratings = lax.dot_general(block_queries, key_rows, (((1,), (1,)), ((), ())), preferred_element_type=jnp.float32) * SOFTMAX_SCALE
        visible = positions[None, :] < block_lengths[:, None]
        row_max = jnp.max(jnp.where(visible, block_ratings, -jnp.inf), axis=1, keepdims=True)
        exponent = jnp.where(visible, jnp.exp(block_ratings - row_max), 0.0)
        normaliser = jnp.sum(exponent, axis=1, keepdims=True)
        weights = exponent.astype(jnp.bfloat16)
        result = jnp.dot(weights, latent, preferred_element_type=jnp.float32) / normaliser
        return result.astype(jnp.bfloat16)

    outputs = lax.map(per_block, (query_rows.reshape(block_count, step_rows, query_rows.shape[1]), row_lengths.reshape(block_count, step_rows)))
    return outputs.reshape(total_rows, LAT)


def reference(queries, latent_cache, block_picks, lengths):
    groups = block_picks.shape[0]
    per_group = queries.shape[0] // groups
    head_count = queries.shape[1]
    feature = queries.shape[2]
    within = jnp.arange(BLOCK, dtype=jnp.int32)

    def per_group_attend(group):
        chosen_blocks = lax.dynamic_index_in_dim(block_picks, group, 0, keepdims=False)
        positions = (chosen_blocks[:, None] * BLOCK + within[None, :]).reshape(-1).astype(jnp.int32)
        key_rows = jnp.take(latent_cache, positions, axis=0)
        first_row = (group * per_group).astype(jnp.int32)
        query_rows = lax.dynamic_slice_in_dim(queries, first_row, per_group, 0).reshape(per_group * head_count, feature)
        row_lengths = jnp.repeat(lax.dynamic_slice_in_dim(lengths, first_row, per_group, 0), head_count)
        return attend(query_rows, key_rows, positions, row_lengths)

    outputs = lax.map(per_group_attend, jnp.arange(groups, dtype=jnp.int32))
    return outputs.reshape(queries.shape[0], head_count, LAT)
```

```python
import functools
import math

import jax
import jax.numpy as jnp
from jax import lax
from jax.experimental import pallas as pl
from jax.experimental.pallas import tpu as pltpu
from jax.sharding import PartitionSpec as P

LAT = 512
BLOCK = 64
TOPK = 32
SOFTMAX_SCALE = 192.0 ** (-0.5)
EXP2_SCALE = SOFTMAX_SCALE * math.log2(math.e)


def pack_kernel(source, cache, out, sem):
    count = out.shape[0] // BLOCK
    copies = [
        pltpu.make_async_copy(
            cache.at[pl.ds(pl.multiple_of(source[i] * BLOCK, BLOCK), BLOCK), :],
            out.at[pl.ds(i * BLOCK, BLOCK), :],
            sem.at[i],
        )
        for i in range(count)
    ]
    for c in copies:
        c.start()
    for c in copies:
        c.wait()


def pack(latent_cache, source):
    count = source.shape[0]
    return pl.pallas_call(
        pack_kernel,
        out_shape=jax.ShapeDtypeStruct((count * BLOCK, latent_cache.shape[1]), latent_cache.dtype),
        in_specs=[
            pl.BlockSpec(memory_space=pltpu.SMEM),
            pl.BlockSpec(memory_space=pltpu.HBM),
        ],
        out_specs=pl.BlockSpec(memory_space=pltpu.HBM),
        scratch_shapes=[pltpu.SemaphoreType.DMA((count,))],
        name="pack",
    )(source, latent_cache)


def attend_kernel(n_buffers, chunks, buffer_ids, slots, lengths, positions, queries, *rest):
    buffers = rest[:n_buffers]
    out, keys, sem = rest[n_buffers:]
    step = pl.program_id(0)
    rows = queries.shape[0] // chunks
    heads = queries.shape[1]

    @pl.when(step == 0)
    def _():
        def begin(j, carry):
            for b in range(n_buffers):
                @pl.when(buffer_ids[j] == b)
                def _():
                    pltpu.make_async_copy(
                        buffers[b].at[pl.ds(pl.multiple_of(slots[j] * BLOCK, BLOCK), BLOCK), :],
                        keys.at[pl.ds(pl.multiple_of(j * BLOCK, BLOCK), BLOCK), :],
                        sem.at[j],
                    ).start()
            return carry

        lax.fori_loop(0, TOPK, begin, 0)

        def finish(j, carry):
            pltpu.make_async_copy(
                buffers[0].at[pl.ds(0, BLOCK), :],
                keys.at[pl.ds(pl.multiple_of(j * BLOCK, BLOCK), BLOCK), :],
                sem.at[j],
            ).wait()
            return carry

        lax.fori_loop(0, TOPK, finish, 0)

    pos = positions[...]

    def scores(i):
        q = queries[i * rows:(i + 1) * rows].reshape(rows * heads, queries.shape[2])
        return lax.dot_general(
            q, keys[...], (((1,), (1,)), ((), ())), preferred_element_type=jnp.float32
        )

    current = scores(0)
    for i in range(chunks):
        following = scores(i + 1) if i + 1 < chunks else None
        weights = []
        sums = []
        for r in range(rows):
            limit = lengths[step * rows * chunks + i * rows + r]
            bias = jnp.where(pos < limit, 0.0, -jnp.inf)
            s = current[r * heads:(r + 1) * heads] + bias
            top = jnp.max(s, axis=1, keepdims=True)
            e = jnp.exp2((s - top) * EXP2_SCALE)
            sums.append(jnp.sum(e, axis=1, keepdims=True))
            weights.append(e.astype(jnp.bfloat16))
        w = jnp.concatenate(weights, axis=0)
        total = jnp.concatenate(sums, axis=0)
        o = jnp.dot(w, keys[:, :LAT], preferred_element_type=jnp.float32)
        o = (o / total).astype(jnp.bfloat16)
        out[i * rows:(i + 1) * rows] = o.reshape(rows, heads, LAT)
        current = following


def attend(queries, buffers, buffer_ids, slots, positions, lengths):
    total, heads, feature = queries.shape
    rows = 4
    chunks = 2
    return pl.pallas_call(
        functools.partial(attend_kernel, len(buffers), chunks),
        grid=(total // rows,),
        out_shape=jax.ShapeDtypeStruct((total, heads, LAT), jnp.bfloat16),
        in_specs=[
            pl.BlockSpec(memory_space=pltpu.SMEM),
            pl.BlockSpec(memory_space=pltpu.SMEM),
            pl.BlockSpec(memory_space=pltpu.SMEM),
            pl.BlockSpec((1, TOPK * BLOCK), lambda i: (0, 0)),
            pl.BlockSpec((rows, heads, feature), lambda i: (i, 0, 0)),
        ]
        + [pl.BlockSpec(memory_space=pltpu.HBM)] * len(buffers),
        out_specs=pl.BlockSpec((rows, heads, LAT), lambda i: (i, 0, 0)),
        scratch_shapes=[
            pltpu.VMEM((TOPK * BLOCK, feature), jnp.bfloat16),
            pltpu.SemaphoreType.DMA((TOPK,)),
        ],
        compiler_params=pltpu.CompilerParams(
            dimension_semantics=("arbitrary",), vmem_limit_bytes=56 * 1024 * 1024
        ),
        name="attend",
    )(buffer_ids, slots, lengths, positions, queries, *buffers)


def relay(own, line, myself):
    def at(z, y, c):
        return (z * 2 + y) * 2 + c

    def send(x, moves):
        return lax.ppermute(x, "ctx", moves)

    def along(d, valid):
        return [
            (at(z, y, c), at(z + d, y, c))
            for z in range(line) for y in range(2) for c in range(2)
            if 0 <= z + d < line and valid(z)
        ]

    def across(valid):
        return [
            (at(z, y, c), at(z, 1 - y, c))
            for z in range(line) for y in range(2) for c in range(2) if valid(z)
        ]

    def partner(valid):
        return [
            (at(z, y, c), at(z, y, 1 - c))
            for z in range(line) for y in range(2) for c in range(2) if valid(z)
        ]

    my_z = myself // 4
    always = lambda z: True
    held = [own, send(own, across(always))]
    rules = [always, always]
    up, down = own, own
    ups, downs = {}, {}
    for t in range(line - 1):
        up = send(up, along(1, lambda z: z - t >= 0))
        down = send(down, along(-1, lambda z: z + t < line))
        has_up = lambda z, t=t: z > t
        has_down = lambda z, t=t: z < line - 1 - t
        if 2 * t + 2 >= line:
            joined = jnp.where(my_z > t, up, down)
            both = lambda z, a=has_up, b=has_down: a(z) or b(z)
            ups[t] = downs[t] = len(held)
            held.append(joined)
            held.append(send(joined, across(both)))
            rules += [both, both]
        else:
            ups[t] = len(held)
            held += [up, send(up, across(has_up))]
            downs[t] = len(held)
            held += [down, send(down, across(has_down))]
            rules += [has_up, has_up, has_down, has_down]
    count = len(held)
    held = held + [send(h, partner(r)) for h, r in zip(held, rules)]
    up_at = jnp.array([0] + [ups[t] for t in range(line - 1)], jnp.int32)
    down_at = jnp.array([0] + [downs[t] for t in range(line - 1)], jnp.int32)

    def where_is(owner):
        z, y, c = owner // 4, (owner // 2) % 2, owner % 2
        gap = my_z - z
        place = jnp.zeros_like(owner)
        for t in range(line - 1):
            place = jnp.where(gap == t + 1, ups[t], place)
            place = jnp.where(gap == -t - 1, downs[t], place)
        place = place + (y != (myself // 2) % 2).astype(jnp.int32)
        return place + count * (c != myself % 2).astype(jnp.int32)

    return held, where_is


def shards(queries, latent_cache, block_picks, lengths):
    ctx_count = lax.axis_size("ctx")
    myself = lax.axis_index("ctx")
    owned = latent_cache.shape[0] // BLOCK
    capacity = max(1, 2 * TOPK // ctx_count)
    union_size = 2 * capacity
    own_picks = block_picks[0]
    owners = own_picks // owned
    all_picks = lax.all_to_all(
        jnp.broadcast_to(block_picks, (ctx_count, TOPK)), "ctx", 0, 0, tiled=True
    ).reshape(-1)

    blocks = myself * owned + jnp.arange(owned, dtype=jnp.int32)
    own_flag = jnp.any(all_picks[None, :] == blocks[:, None], axis=1)
    earlier = blocks[None, :] < blocks[:, None]
    rank = jnp.sum((earlier & own_flag[None, :]).astype(jnp.int32), axis=1)
    slot_ids = jnp.arange(union_size, dtype=jnp.int32)
    matches = (rank[None, :] == slot_ids[:, None]) & own_flag[None, :]
    source = jnp.sum(matches.astype(jnp.int32) * jnp.arange(owned, dtype=jnp.int32)[None, :], axis=1)
    own = pack(latent_cache, source)

    named = jnp.zeros((TOPK,), jnp.int32)
    for k in range(owned):
        block = owners * owned + k
        seen = jnp.any(all_picks[None, :] == block[:, None], axis=1) & (block < own_picks)
        named = named + seen.astype(jnp.int32)

    if ctx_count % 4 == 0 and ctx_count // 4 <= 4:
        buffers, where_is = relay(own, ctx_count // 4, myself)
        buffer_ids, slots = where_is(owners), named
    else:
        buffers = [lax.all_gather(own, "ctx", axis=0, tiled=True)]
        buffer_ids, slots = jnp.zeros_like(owners), owners * union_size + named
    within = jnp.arange(BLOCK, dtype=jnp.int32)
    positions = (own_picks[:, None] * BLOCK + within[None, :]).reshape(1, -1)
    return attend(queries, buffers, buffer_ids, slots, positions, lengths)


def solution(mesh):
    placed = (
        P(("groups", "ctx"), None, None),
        P(("groups", "ctx"), None),
        P(("groups", "ctx"), None),
        P(("groups", "ctx")),
    )
    return jax.shard_map(
        shards,
        mesh=mesh,
        in_specs=placed,
        out_specs=P(("groups", "ctx"), None, None),
        check_vma=False,
    )
```

```python
import functools
import math

import jax
import jax.numpy as jnp
from jax import lax
from jax.experimental import pallas as pl
from jax.experimental.pallas import tpu as pltpu
from jax.sharding import PartitionSpec as P

LAT = 512
BLOCK = 64
TOPK = 32
SOFTMAX_SCALE = 192.0 ** (-0.5)
EXP2_SCALE = SOFTMAX_SCALE * math.log2(math.e)


def pack_kernel(source, cache, out, raw, sem):
    count = out.shape[0]
    copies = [
        pltpu.make_async_copy(
            cache.at[pl.ds(pl.multiple_of(source[i] * BLOCK, BLOCK), BLOCK), :],
            raw.at[i],
            sem.at[i],
        )
        for i in range(count)
    ]
    for c in copies:
        c.start()
    for c in copies:
        c.wait()
    out[:, :BLOCK, :] = raw[:, :, :LAT]
    tail = raw[:, :, LAT:].astype(jnp.float32)
    width = tail.shape[2]
    pieces = LAT // width
    rows = BLOCK // pieces
    folded = jnp.concatenate([tail[:, i * rows:(i + 1) * rows] for i in range(pieces)], axis=2)
    out[:, BLOCK:, :] = folded.astype(out.dtype)


def pack(latent_cache, source):
    count = source.shape[0]
    feature = latent_cache.shape[1]
    rows = BLOCK + BLOCK * (feature - LAT) // LAT
    return pl.pallas_call(
        pack_kernel,
        out_shape=jax.ShapeDtypeStruct((count, rows, LAT), latent_cache.dtype),
        in_specs=[
            pl.BlockSpec(memory_space=pltpu.SMEM),
            pl.BlockSpec(memory_space=pltpu.HBM),
        ],
        out_specs=pl.BlockSpec(memory_space=pltpu.VMEM),
        scratch_shapes=[
            pltpu.VMEM((count, BLOCK, feature), latent_cache.dtype),
            pltpu.SemaphoreType.DMA((count,)),
        ],
        name="pack",
    )(source, latent_cache)


def attend_kernel(n_buffers, chunks, buffer_ids, slots, lengths, positions, queries, *rest):
    buffers = rest[:n_buffers]
    out, keys, folded, sem = rest[n_buffers:]
    step = pl.program_id(0)
    rows = queries.shape[0] // chunks
    heads = queries.shape[2]
    tail = keys.shape[1] - LAT

    def fetch(b, j, slot):
        spot = pl.ds(pl.multiple_of(j * BLOCK, BLOCK), BLOCK)
        return (
            pltpu.make_async_copy(
                buffers[b].at[slot, pl.ds(0, BLOCK)], keys.at[spot, pl.ds(0, LAT)], sem.at[0, j]
            ),
            pltpu.make_async_copy(
                buffers[b].at[slot, pl.ds(BLOCK, folded.shape[1])], folded.at[j], sem.at[1, j]
            ),
        )

    @pl.when(step == 0)
    def _():
        def begin(j, carry):
            for b in range(n_buffers):
                @pl.when(buffer_ids[j] == b)
                def _():
                    for c in fetch(b, j, slots[j]):
                        c.start()
            return carry

        lax.fori_loop(0, TOPK, begin, 0)

        def finish(j, carry):
            for c in fetch(0, j, 0):
                c.wait()
            return carry

        lax.fori_loop(0, TOPK, finish, 0)
        wide = folded[...].astype(jnp.float32)
        parts = [wide[:, :, i * tail:(i + 1) * tail] for i in range(LAT // tail)]
        rope = jnp.concatenate(parts, axis=1).astype(keys.dtype)
        keys[:, LAT:] = rope.reshape(keys.shape[0], tail)

    pos = positions[...]

    def scores(i):
        q = jnp.concatenate([queries[i * rows + r].T for r in range(rows)], axis=0)
        return lax.dot_general(
            q, keys[...], (((1,), (1,)), ((), ())), preferred_element_type=jnp.float32
        )

    current = scores(0)
    for i in range(chunks):
        following = scores(i + 1) if i + 1 < chunks else None
        weights = []
        sums = []
        for r in range(rows):
            limit = lengths[step * rows * chunks + i * rows + r]
            bias = jnp.where(pos < limit, 0.0, -jnp.inf)
            s = current[r * heads:(r + 1) * heads] + bias
            top = jnp.max(s, axis=1, keepdims=True)
            e = jnp.exp2((s - top) * EXP2_SCALE)
            sums.append(jnp.sum(e, axis=1, keepdims=True))
            weights.append(e.astype(jnp.bfloat16))
        w = jnp.concatenate(weights, axis=0)
        total = jnp.concatenate(sums, axis=0)
        o = jnp.dot(w, keys[:, :LAT], preferred_element_type=jnp.float32)
        o = (o / total).astype(jnp.bfloat16)
        out[i * rows:(i + 1) * rows] = o.reshape(rows, heads, LAT)
        current = following


def attend(queries, buffers, buffer_ids, slots, positions, lengths):
    total, heads, feature = queries.shape
    queries = queries.transpose(0, 2, 1)
    rows = 4
    chunks = 2
    return pl.pallas_call(
        functools.partial(attend_kernel, len(buffers), chunks),
        grid=(total // rows,),
        out_shape=jax.ShapeDtypeStruct((total, heads, LAT), jnp.bfloat16),
        in_specs=[
            pl.BlockSpec(memory_space=pltpu.SMEM),
            pl.BlockSpec(memory_space=pltpu.SMEM),
            pl.BlockSpec(memory_space=pltpu.SMEM),
            pl.BlockSpec((1, TOPK * BLOCK), lambda i: (0, 0)),
            pl.BlockSpec((rows, feature, heads), lambda i: (i, 0, 0)),
        ]
        + [pl.BlockSpec(memory_space=pltpu.HBM)] * len(buffers),
        out_specs=pl.BlockSpec((rows, heads, LAT), lambda i: (i, 0, 0)),
        scratch_shapes=[
            pltpu.VMEM((TOPK * BLOCK, feature), jnp.bfloat16),
            pltpu.VMEM((TOPK, buffers[0].shape[1] - BLOCK, LAT), jnp.bfloat16),
            pltpu.SemaphoreType.DMA((2, TOPK)),
        ],
        compiler_params=pltpu.CompilerParams(
            dimension_semantics=("arbitrary",), vmem_limit_bytes=56 * 1024 * 1024
        ),
        name="attend",
    )(buffer_ids, slots, lengths, positions, queries, *buffers)


def relay(own, myself):
    line = 4
    union_size = own.shape[0]
    half = union_size // 2
    my_z, my_y, my_c = myself // 4, (myself // 2) % 2, myself % 2
    end = (my_z == 0) | (my_z == line - 1)

    def at(z, y, c):
        return (z * 2 + y) * 2 + c

    places = [(z, y, c) for z in range(line) for y in range(2) for c in range(2)]

    def along(x, steps):
        moves = [(at(z, y, c), at(z + steps[z], y, c)) for z, y, c in places if z in steps]
        return lax.ppermute(x, "ctx", moves)

    def across(x, zs=range(line)):
        return lax.ppermute(x, "ctx", [(at(z, y, c), at(z, 1 - y, c)) for z, y, c in places if z in zs])

    def partner(x):
        return lax.ppermute(x, "ctx", [(at(z, y, c), at(z, y, 1 - c)) for z, y, c in places])

    tie = lax.optimization_barrier
    up0 = along(own, {0: 1, 1: 1, 2: 1})
    down0 = along(own, {1: -1, 2: -1, 3: -1})
    pair0 = across(own)
    own_p = partner(own)
    up0, down0, pair0, own_p = tie((up0, down0, pair0, own_p))

    up1 = along(up0, {1: 1, 2: 1})
    down1 = along(down0, {1: -1, 2: -1})
    pair1 = across(jnp.where(my_z % 2 == 0, down0, up0))
    up0_p, down0_p, pair0_p = partner(up0), partner(down0), partner(pair0)
    up1, down1, pair1, up0_p, down0_p, pair0_p = tie((up1, down1, pair1, up0_p, down0_p, pair0_p))

    far1 = jnp.where(my_z >= 2, up1, down1)
    up2 = along(jnp.where(my_z == 1, pair0, up1), {1: 1, 2: 1})
    down2 = along(jnp.where(my_z == 2, pair0, down1), {1: -1, 2: -1})
    pair2 = across(far1)
    far1_p, pair1_p = partner(far1), partner(pair1)
    up2, down2, pair2, far1_p, pair1_p = tie((up2, down2, pair2, far1_p, pair1_p))

    far2 = jnp.where(my_z >= 2, up2, down2)
    last_a = across(far2[:half], (0, line - 1))
    last_b = along(pair2[half:], {1: -1, 2: 1})
    far2_p, pair2_p = partner(far2), partner(pair2)
    last_a_p, last_b_p = partner(last_a), partner(last_b)
    held = [own, pair0, up0, down0, far1, pair1, far2, pair2, last_a, last_b]
    held_p = [own_p, pair0_p, up0_p, down0_p, far1_p, pair1_p, far2_p, pair2_p, last_a_p, last_b_p]

    def where_is(owner, slot):
        z, y, c = owner // 4, (owner // 2) % 2, owner % 2
        gap = z - my_z
        same = jnp.where(gap == 0, 0, jnp.where(gap == -1, 2, jnp.where(gap == 1, 3, 4)))
        same = jnp.where(jnp.abs(gap) == 3, 6, same)
        late = slot >= half
        opposite = jnp.where(end, jnp.where(late, 9, 8), 6)
        other = jnp.where(z == my_z ^ 1, 5, jnp.where(z == my_z ^ 2, 7, opposite))
        other = jnp.where(gap == 0, 1, other)
        buffer = jnp.where(y == my_y, same, other)
        slot = jnp.where((buffer == 9) & late, slot - half, slot)
        return buffer + len(held) * (c != my_c).astype(jnp.int32), slot

    return held + held_p, where_is


def shards(queries, latent_cache, block_picks, lengths):
    ctx_count = lax.axis_size("ctx")
    myself = lax.axis_index("ctx")
    owned = latent_cache.shape[0] // BLOCK
    capacity = max(1, 2 * TOPK // ctx_count)
    union_size = 2 * capacity
    own_picks = block_picks[0]
    owners = own_picks // owned
    all_picks = lax.all_to_all(
        jnp.broadcast_to(block_picks, (ctx_count, TOPK)), "ctx", 0, 0, tiled=True
    ).reshape(-1)

    blocks = myself * owned + jnp.arange(owned, dtype=jnp.int32)
    own_flag = jnp.any(all_picks[None, :] == blocks[:, None], axis=1)
    earlier = blocks[None, :] < blocks[:, None]
    rank = jnp.sum((earlier & own_flag[None, :]).astype(jnp.int32), axis=1)
    slot_ids = jnp.arange(union_size, dtype=jnp.int32)
    matches = (rank[None, :] == slot_ids[:, None]) & own_flag[None, :]
    source = jnp.sum(matches.astype(jnp.int32) * jnp.arange(owned, dtype=jnp.int32)[None, :], axis=1)
    own = pack(latent_cache, source)

    named = jnp.zeros((TOPK,), jnp.int32)
    for k in range(owned):
        block = owners * owned + k
        seen = jnp.any(all_picks[None, :] == block[:, None], axis=1) & (block < own_picks)
        named = named + seen.astype(jnp.int32)

    if ctx_count == 16:
        buffers, where_is = relay(own, myself)
        buffer_ids, slots = where_is(owners, named)
    else:
        buffers = [lax.all_gather(own, "ctx", axis=0, tiled=True)]
        buffer_ids, slots = jnp.zeros_like(owners), owners * union_size + named
    within = jnp.arange(BLOCK, dtype=jnp.int32)
    positions = (own_picks[:, None] * BLOCK + within[None, :]).reshape(1, -1)
    return attend(queries, buffers, buffer_ids, slots, positions, lengths)


def solution(mesh):
    placed = (
        P(("groups", "ctx"), None, None),
        P(("groups", "ctx"), None),
        P(("groups", "ctx"), None),
        P(("groups", "ctx")),
    )
    return jax.shard_map(
        shards,
        mesh=mesh,
        in_specs=placed,
        out_specs=P(("groups", "ctx"), None, None),
        check_vma=False,
    )
```

```python
import functools
import math

import jax
import jax.numpy as jnp
from jax import lax
from jax.experimental import pallas as pl
from jax.experimental.pallas import tpu as pltpu
from jax.sharding import PartitionSpec as P

LAT = 512
BLOCK = 64
TOPK = 32
SOFTMAX_SCALE = 192.0 ** (-0.5)
EXP2_SCALE = SOFTMAX_SCALE * math.log2(math.e)

CHUNK = 4
LOW = -1e30


def pack_kernel(source, cache, out, raw, sem):
    count = out.shape[0]
    copies = [
        pltpu.make_async_copy(
            cache.at[pl.ds(pl.multiple_of(source[i] * BLOCK, BLOCK), BLOCK), :],
            raw.at[i],
            sem.at[i],
        )
        for i in range(count)
    ]
    for c in copies:
        c.start()
    for c in copies:
        c.wait()
    out[:, :BLOCK, :] = raw[:, :, :LAT]
    tail = raw[:, :, LAT:].astype(jnp.float32)
    width = tail.shape[2]
    pieces = LAT // width
    rows = BLOCK // pieces
    folded = jnp.concatenate([tail[:, i * rows:(i + 1) * rows] for i in range(pieces)], axis=2)
    out[:, BLOCK:, :] = folded.astype(out.dtype)


def pack(latent_cache, source):
    count = source.shape[0]
    feature = latent_cache.shape[1]
    rows = BLOCK + BLOCK * (feature - LAT) // LAT
    return pl.pallas_call(
        pack_kernel,
        out_shape=jax.ShapeDtypeStruct((count, rows, LAT), latent_cache.dtype),
        in_specs=[
            pl.BlockSpec(memory_space=pltpu.SMEM),
            pl.BlockSpec(memory_space=pltpu.HBM),
        ],
        out_specs=pl.BlockSpec(memory_space=pltpu.VMEM),
        scratch_shapes=[
            pltpu.VMEM((count, BLOCK, feature), latent_cache.dtype),
            pltpu.SemaphoreType.DMA((count,)),
        ],
        name="pack",
    )(source, latent_cache)


def attend_kernel(n_buffers, first, last, heads, buffer_ids, slots, count, lengths, positions, queries, *rest):
    buffers = rest[:n_buffers]
    rest = rest[n_buffers:]
    if not first:
        acc_in, top_in, sum_in = rest[:3]
        rest = rest[3:]
    if last:
        out, keys, folded, rows_q, acc, top, total, sem = rest
    else:
        acc, top, total, keys, folded, rows_q, sem = rest
    step = pl.program_id(0)
    rows = queries.shape[0]
    tail = keys.shape[1] - LAT
    chunks = (count[0] + CHUNK - 1) // CHUNK
    loaded = chunks * CHUNK

    def fetch(b, j, slot):
        spot = pl.ds(pl.multiple_of(j * BLOCK, BLOCK), BLOCK)
        return (
            pltpu.make_async_copy(
                buffers[b].at[slot, pl.ds(0, BLOCK)], keys.at[spot, pl.ds(0, LAT)], sem.at[0, j]
            ),
            pltpu.make_async_copy(
                buffers[b].at[slot, pl.ds(BLOCK, folded.shape[1])], folded.at[j], sem.at[1, j]
            ),
        )

    @pl.when(step == 0)
    def _():
        def begin(j, carry):
            for b in range(n_buffers):
                @pl.when(buffer_ids[j] == b)
                def _():
                    for c in fetch(b, j, slots[j]):
                        c.start()
            return carry

        lax.fori_loop(0, loaded, begin, 0)

        def finish(j, carry):
            for c in fetch(0, j, 0):
                c.wait()
            wide = folded[j].astype(jnp.float32)
            parts = [wide[:, i * tail:(i + 1) * tail] for i in range(LAT // tail)]
            spot = pl.ds(pl.multiple_of(j * BLOCK, BLOCK), BLOCK)
            keys[spot, LAT:] = jnp.concatenate(parts, axis=0).astype(keys.dtype)
            return carry

        lax.fori_loop(0, loaded, finish, 0)

    for r in range(rows):
        rows_q[r * heads:(r + 1) * heads, :] = queries[r].T
    if first:
        acc[...] = jnp.zeros(acc.shape, acc.dtype)
        top[...] = jnp.full(top.shape, LOW, top.dtype)
        total[...] = jnp.zeros(total.shape, total.dtype)
    else:
        acc[...] = acc_in[...]
        top[...] = top_in[...]
        total[...] = sum_in[...]

    group = rows // 2
    span = group * heads

    def chunk(i, carry):
        spot = pl.ds(pl.multiple_of(i * CHUNK * BLOCK, CHUNK * BLOCK), CHUNK * BLOCK)
        pos = positions[i]
        key = keys[spot, :]
        raw = [
            lax.dot_general(
                rows_q[g * span:(g + 1) * span, :], key, (((1,), (1,)), ((), ())),
                preferred_element_type=jnp.float32,
            )
            for g in range(2)
        ]
        for g in range(2):
            at = slice(g * span, (g + 1) * span)
            parts = []
            for r in range(group):
                limit = lengths[step * rows + g * group + r]
                bias = jnp.where(pos < limit, 0.0, -jnp.inf)
                parts.append(raw[g][r * heads:(r + 1) * heads] + bias)
            s = jnp.concatenate(parts, axis=0)
            old = top[at, :]
            new = jnp.maximum(old, jnp.max(s, axis=1, keepdims=True))
            scale = jnp.exp2((old - new) * EXP2_SCALE)
            e = jnp.exp2((s - new[:, :1]) * EXP2_SCALE)
            top[at, :] = new
            total[at, :] = total[at, :] * scale + jnp.sum(e, axis=1, keepdims=True)
            o = jnp.dot(e.astype(jnp.bfloat16), key[:, :LAT], preferred_element_type=jnp.float32)
            acc[at, :] = acc[at, :] * scale[:, :1] + o
        return carry

    lax.fori_loop(0, chunks, chunk, 0)
    if last:
        o = (acc[...] / total[:, :1]).astype(jnp.bfloat16)
        out[...] = o.reshape(out.shape)


def attend(queries, buffers, plan, lengths, state, last):
    buffer_ids, slots, count, positions = plan
    total, heads, feature = queries.shape
    queries = queries.transpose(0, 2, 1)
    rows = 4
    wide = 128
    row_spec = lambda n: pl.BlockSpec((rows * heads, n), lambda i: (i, 0))
    state_specs = [row_spec(LAT), row_spec(wide), row_spec(wide)]
    block_rows = [pltpu.VMEM((rows * heads, n), jnp.float32) for n in (LAT, wide, wide)]
    first = state is None
    smem = pl.BlockSpec(memory_space=pltpu.SMEM)
    scratch = [
        pltpu.VMEM((TOPK * BLOCK, feature), jnp.bfloat16),
        pltpu.VMEM((TOPK, buffers[0].shape[1] - BLOCK, LAT), jnp.bfloat16),
        pltpu.VMEM((rows * heads, feature), jnp.bfloat16),
    ]
    if last:
        out_shape = jax.ShapeDtypeStruct((total, heads, LAT), jnp.bfloat16)
        out_specs = pl.BlockSpec((rows, heads, LAT), lambda i: (i, 0, 0))
        scratch += block_rows
    else:
        out_shape = [jax.ShapeDtypeStruct((total * heads, n), jnp.float32) for n in (LAT, wide, wide)]
        out_specs = state_specs
    scratch.append(pltpu.SemaphoreType.DMA((2, TOPK)))
    return pl.pallas_call(
        functools.partial(attend_kernel, len(buffers), first, last, heads),
        grid=(total // rows,),
        out_shape=out_shape,
        in_specs=[
            smem, smem, smem, smem,
            pl.BlockSpec(positions.shape, lambda i: (0, 0, 0)),
            pl.BlockSpec((rows, feature, heads), lambda i: (i, 0, 0)),
        ]
        + [pl.BlockSpec(memory_space=pltpu.HBM)] * len(buffers)
        + ([] if first else state_specs),
        out_specs=out_specs,
        scratch_shapes=scratch,
        compiler_params=pltpu.CompilerParams(
            dimension_semantics=("arbitrary",), vmem_limit_bytes=40 * 1024 * 1024
        ),
        name="attend",
    )(buffer_ids, slots, count, lengths, positions, queries, *buffers, *([] if first else state))


def make_plan(member, buffer_ids, slots, picks):
    order = jnp.arange(TOPK, dtype=jnp.int32)
    before = (order[None, :] < order[:, None]) & member[None, :]
    dest = jnp.sum(before.astype(jnp.int32), axis=1)
    chosen = (dest[None, :] == order[:, None]) & member[None, :]
    put = lambda v: jnp.sum(jnp.where(chosen, v[None, :], 0), axis=1)
    count = jnp.sum(member.astype(jnp.int32)).reshape(1)
    base = jnp.where(order < count, put(picks) * BLOCK, 1 << 30)
    within = jnp.arange(BLOCK, dtype=jnp.int32)
    positions = (base[:, None] + within[None, :]).reshape(TOPK // CHUNK, 1, CHUNK * BLOCK)
    return put(buffer_ids), put(slots), count, positions


def relay_attend(own, myself, owners, named, own_picks, queries, lengths):
    line = 4
    union_size = own.shape[0]
    half = union_size // 2
    my_z, my_y, my_c = myself // 4, (myself // 2) % 2, myself % 2
    end = (my_z == 0) | (my_z == line - 1)

    def at(z, y, c):
        return (z * 2 + y) * 2 + c

    places = [(z, y, c) for z in range(line) for y in range(2) for c in range(2)]

    def along(x, steps):
        moves = [(at(z, y, c), at(z + steps[z], y, c)) for z, y, c in places if z in steps]
        return lax.ppermute(x, "ctx", moves)

    def across(x, zs=range(line)):
        return lax.ppermute(x, "ctx", [(at(z, y, c), at(z, 1 - y, c)) for z, y, c in places if z in zs])

    def partner(x):
        return lax.ppermute(x, "ctx", [(at(z, y, c), at(z, y, 1 - c)) for z, y, c in places])

    tie = lax.optimization_barrier

    held = 10

    def where_is(owner, slot):
        z, y, c = owner // 4, (owner // 2) % 2, owner % 2
        gap = z - my_z
        same = jnp.where(gap == 0, 0, jnp.where(gap == -1, 2, jnp.where(gap == 1, 3, 4)))
        same = jnp.where(jnp.abs(gap) == 3, 6, same)
        late = slot >= half
        opposite = jnp.where(end, jnp.where(late, 9, 8), 6)
        other = jnp.where(z == my_z ^ 1, 5, jnp.where(z == my_z ^ 2, 7, opposite))
        other = jnp.where(gap == 0, 1, other)
        buffer = jnp.where(y == my_y, same, other)
        slot = jnp.where((buffer == 9) & late, slot - half, slot)
        return buffer + held * (c != my_c).astype(jnp.int32), slot

    buffer_ids, slots = where_is(owners, named)
    sets = ((0, 1, 2, 3, 4, 5, 10, 11, 12, 13), (0, 6, 7, 14, 15), (0, 8, 9, 16, 17, 18, 19))
    plans = []
    for p, ids in enumerate(sets):
        member = jnp.zeros((TOPK,), bool)
        local = jnp.zeros((TOPK,), jnp.int32)
        for k, b in enumerate(ids):
            if p == 0 or k > 0:
                hit = buffer_ids == b
                member = member | hit
                local = jnp.where(hit, k, local)
        plans.append(make_plan(member, local, slots, own_picks))

    up0 = along(own, {0: 1, 1: 1, 2: 1})
    down0 = along(own, {1: -1, 2: -1, 3: -1})
    pair0 = across(own)
    own_p = partner(own)
    up0, down0, pair0, own_p, plans = tie((up0, down0, pair0, own_p, plans))

    up1 = along(up0, {1: 1, 2: 1})
    down1 = along(down0, {1: -1, 2: -1})
    pair1 = across(jnp.where(my_z % 2 == 0, down0, up0))
    up0_p, down0_p, pair0_p = partner(up0), partner(down0), partner(pair0)
    up1, down1, pair1, up0_p, down0_p, pair0_p = tie((up1, down1, pair1, up0_p, down0_p, pair0_p))

    far1 = jnp.where(my_z >= 2, up1, down1)
    up2 = along(jnp.where(my_z == 1, pair0, up1), {1: 1, 2: 1})
    down2 = along(jnp.where(my_z == 2, pair0, down1), {1: -1, 2: -1})
    pair2 = across(far1)
    far1_p, pair1_p = partner(far1), partner(pair1)
    near = [own, pair0, up0, down0, far1, pair1, own_p, pair0_p, up0_p, down0_p]
    state = attend(queries, near, plans[0], lengths, None, False)
    up2, down2, pair2, far1_p, pair1_p, state = tie((up2, down2, pair2, far1_p, pair1_p, state))

    far2 = jnp.where(my_z >= 2, up2, down2)
    last_a = across(far2[:half], (0, line - 1))
    last_b = along(pair2[half:], {1: -1, 2: 1})
    far2_p, pair2_p = partner(far2), partner(pair2)
    state = attend(queries, [own, far2, pair2, far1_p, pair1_p], plans[1], lengths, state, False)
    last_a, last_b, far2_p, pair2_p, state = tie((last_a, last_b, far2_p, pair2_p, state))
    last_a_p, last_b_p = partner(last_a), partner(last_b)
    rest = [own, last_a, last_b, far2_p, pair2_p, last_a_p, last_b_p]
    return attend(queries, rest, plans[2], lengths, state, True)


def shards(queries, latent_cache, block_picks, lengths):
    ctx_count = lax.axis_size("ctx")
    myself = lax.axis_index("ctx")
    owned = latent_cache.shape[0] // BLOCK
    capacity = max(1, 2 * TOPK // ctx_count)
    union_size = 2 * capacity
    own_picks = block_picks[0]
    owners = own_picks // owned
    all_picks = lax.all_to_all(
        jnp.broadcast_to(block_picks, (ctx_count, TOPK)), "ctx", 0, 0, tiled=True
    ).reshape(-1)

    blocks = myself * owned + jnp.arange(owned, dtype=jnp.int32)
    own_flag = jnp.any(all_picks[None, :] == blocks[:, None], axis=1)
    earlier = blocks[None, :] < blocks[:, None]
    rank = jnp.sum((earlier & own_flag[None, :]).astype(jnp.int32), axis=1)
    slot_ids = jnp.arange(union_size, dtype=jnp.int32)
    matches = (rank[None, :] == slot_ids[:, None]) & own_flag[None, :]
    source = jnp.sum(matches.astype(jnp.int32) * jnp.arange(owned, dtype=jnp.int32)[None, :], axis=1)
    own = pack(latent_cache, source)

    named = jnp.zeros((TOPK,), jnp.int32)
    for k in range(owned):
        block = owners * owned + k
        seen = jnp.any(all_picks[None, :] == block[:, None], axis=1) & (block < own_picks)
        named = named + seen.astype(jnp.int32)

    if ctx_count == 16:
        return relay_attend(own, myself, owners, named, own_picks, queries, lengths)
    gathered = lax.all_gather(own, "ctx", axis=0, tiled=True)
    everything = jnp.ones((TOPK,), bool)
    plan = make_plan(everything, jnp.zeros_like(owners), owners * union_size + named, own_picks)
    return attend(queries, [gathered], plan, lengths, None, True)


def solution(mesh):
    placed = (
        P(("groups", "ctx"), None, None),
        P(("groups", "ctx"), None),
        P(("groups", "ctx"), None),
        P(("groups", "ctx")),
    )
    return jax.shard_map(
        shards,
        mesh=mesh,
        in_specs=placed,
        out_specs=P(("groups", "ctx"), None, None),
        check_vma=False,
    )
```

```python
import functools
import math

import jax
import jax.numpy as jnp
from jax import lax
from jax.experimental import pallas as pl
from jax.experimental.pallas import tpu as pltpu
from jax.sharding import PartitionSpec as P

LAT = 512
BLOCK = 64
TOPK = 32
SOFTMAX_SCALE = 192.0 ** (-0.5)
EXP2_SCALE = SOFTMAX_SCALE * math.log2(math.e)

ROWS = 4


def pack_kernel(source, cache, out, raw, sem):
    count = out.shape[0]
    copies = [
        pltpu.make_async_copy(
            cache.at[pl.ds(pl.multiple_of(source[i] * BLOCK, BLOCK), BLOCK), :],
            raw.at[i],
            sem.at[i],
        )
        for i in range(count)
    ]
    for c in copies:
        c.start()
    for c in copies:
        c.wait()
    out[:, :BLOCK, :] = raw[:, :, :LAT]
    tail = raw[:, :, LAT:].astype(jnp.float32)
    width = tail.shape[2]
    pieces = LAT // width
    rows = BLOCK // pieces
    folded = jnp.concatenate([tail[:, i * rows:(i + 1) * rows] for i in range(pieces)], axis=2)
    out[:, BLOCK:, :] = folded.astype(out.dtype)


def pack(latent_cache, source):
    count = source.shape[0]
    feature = latent_cache.shape[1]
    rows = BLOCK + BLOCK * (feature - LAT) // LAT
    return pl.pallas_call(
        pack_kernel,
        out_shape=jax.ShapeDtypeStruct((count, rows, LAT), latent_cache.dtype),
        in_specs=[
            pl.BlockSpec(memory_space=pltpu.SMEM),
            pl.BlockSpec(memory_space=pltpu.HBM),
        ],
        out_specs=pl.BlockSpec(memory_space=pltpu.VMEM),
        scratch_shapes=[
            pltpu.VMEM((count, BLOCK, feature), latent_cache.dtype),
            pltpu.SemaphoreType.DMA((count,)),
        ],
        name="pack",
    )(source, latent_cache)


def attend_kernel(n_buffers, chunks, buffer_ids, slots, lengths, positions, queries, *rest):
    buffers = rest[:n_buffers]
    out, keys, folded, sem = rest[n_buffers:]
    step = pl.program_id(0)
    rows = queries.shape[0] // chunks
    heads = queries.shape[2]
    tail = keys.shape[1] - LAT

    def fetch(b, j, slot):
        spot = pl.ds(pl.multiple_of(j * BLOCK, BLOCK), BLOCK)
        return (
            pltpu.make_async_copy(
                buffers[b].at[slot, pl.ds(0, BLOCK)], keys.at[spot, pl.ds(0, LAT)], sem.at[0, j]
            ),
            pltpu.make_async_copy(
                buffers[b].at[slot, pl.ds(BLOCK, folded.shape[1])], folded.at[j], sem.at[1, j]
            ),
        )

    @pl.when(step == 0)
    def _():
        def begin(j, carry):
            for b in range(n_buffers):
                @pl.when(buffer_ids[j] == b)
                def _():
                    for c in fetch(b, j, slots[j]):
                        c.start()
            return carry

        lax.fori_loop(0, TOPK, begin, 0)

        def finish(j, carry):
            for c in fetch(0, j, 0):
                c.wait()
            return carry

        lax.fori_loop(0, TOPK, finish, 0)
        wide = folded[...].astype(jnp.float32)
        parts = [wide[:, :, i * tail:(i + 1) * tail] for i in range(LAT // tail)]
        rope = jnp.concatenate(parts, axis=1).astype(keys.dtype)
        keys[:, LAT:] = rope.reshape(keys.shape[0], tail)

    pos = positions[...]

    def scores(i):
        q = jnp.concatenate([queries[i * rows + r].T for r in range(rows)], axis=0)
        return lax.dot_general(
            q, keys[...], (((1,), (1,)), ((), ())), preferred_element_type=jnp.float32
        )

    current = scores(0)
    for i in range(chunks):
        following = scores(i + 1) if i + 1 < chunks else None
        weights = []
        sums = []
        for r in range(rows):
            limit = lengths[step * rows * chunks + i * rows + r]
            bias = jnp.where(pos < limit, 0.0, -jnp.inf)
            s = current[r * heads:(r + 1) * heads] + bias
            top = jnp.max(s, axis=1, keepdims=True)
            e = jnp.exp2((s - top) * EXP2_SCALE)
            sums.append(jnp.sum(e, axis=1, keepdims=True))
            weights.append(e.astype(jnp.bfloat16))
        w = jnp.concatenate(weights, axis=0)
        total = jnp.concatenate(sums, axis=0)
        o = jnp.dot(w, keys[:, :LAT], preferred_element_type=jnp.float32)
        o = (o / total).astype(jnp.bfloat16)
        out[i * rows:(i + 1) * rows] = o.reshape(rows, heads, LAT)
        current = following


def attend(queries, buffers, buffer_ids, slots, positions, lengths):
    total, heads, feature = queries.shape
    queries = queries.transpose(0, 2, 1)
    rows = next(r for r in (ROWS, 4, 1) if total % r == 0)
    chunks = max(1, rows // 2)
    return pl.pallas_call(
        functools.partial(attend_kernel, len(buffers), chunks),
        grid=(total // rows,),
        out_shape=jax.ShapeDtypeStruct((total, heads, LAT), jnp.bfloat16),
        in_specs=[
            pl.BlockSpec(memory_space=pltpu.SMEM),
            pl.BlockSpec(memory_space=pltpu.SMEM),
            pl.BlockSpec(memory_space=pltpu.SMEM),
            pl.BlockSpec((1, TOPK * BLOCK), lambda i: (0, 0)),
            pl.BlockSpec((rows, feature, heads), lambda i: (i, 0, 0)),
        ]
        + [pl.BlockSpec(memory_space=pltpu.HBM)] * len(buffers),
        out_specs=pl.BlockSpec((rows, heads, LAT), lambda i: (i, 0, 0)),
        scratch_shapes=[
            pltpu.VMEM((TOPK * BLOCK, feature), jnp.bfloat16),
            pltpu.VMEM((TOPK, buffers[0].shape[1] - BLOCK, LAT), jnp.bfloat16),
            pltpu.SemaphoreType.DMA((2, TOPK)),
        ],
        compiler_params=pltpu.CompilerParams(
            dimension_semantics=("arbitrary",), vmem_limit_bytes=56 * 1024 * 1024
        ),
        name="attend",
    )(buffer_ids, slots, lengths, positions, queries, *buffers)


def relay(own, myself, owners, named, positions):
    line = 4
    union_size = own.shape[0]
    half = union_size // 2
    my_z, my_y, my_c = myself // 4, (myself // 2) % 2, myself % 2
    end = (my_z == 0) | (my_z == line - 1)

    def at(z, y, c):
        return (z * 2 + y) * 2 + c

    places = [(z, y, c) for z in range(line) for y in range(2) for c in range(2)]

    def along(x, steps):
        moves = [(at(z, y, c), at(z + steps[z], y, c)) for z, y, c in places if z in steps]
        return lax.ppermute(x, "ctx", moves)

    def across(x, zs=range(line)):
        return lax.ppermute(x, "ctx", [(at(z, y, c), at(z, 1 - y, c)) for z, y, c in places if z in zs])

    def partner(x):
        return lax.ppermute(x, "ctx", [(at(z, y, c), at(z, y, 1 - c)) for z, y, c in places])

    tie = lax.optimization_barrier
    count = 10

    def where_is(owner, slot):
        z, y, c = owner // 4, (owner // 2) % 2, owner % 2
        gap = z - my_z
        same = jnp.where(gap == 0, 0, jnp.where(gap == -1, 2, jnp.where(gap == 1, 3, 4)))
        same = jnp.where(jnp.abs(gap) == 3, 6, same)
        late = slot >= half
        opposite = jnp.where(end, jnp.where(late, 9, 8), 6)
        other = jnp.where(z == my_z ^ 1, 5, jnp.where(z == my_z ^ 2, 7, opposite))
        other = jnp.where(gap == 0, 1, other)
        buffer = jnp.where(y == my_y, same, other)
        slot = jnp.where((buffer == 9) & late, slot - half, slot)
        return buffer + count * (c != my_c).astype(jnp.int32), slot

    plan = (*where_is(owners, named), positions)
    up0 = along(own, {0: 1, 1: 1, 2: 1})
    down0 = along(own, {1: -1, 2: -1, 3: -1})
    pair0 = across(own)
    own_p = partner(own)
    up0, down0, pair0, own_p, plan = tie((up0, down0, pair0, own_p, plan))

    up1 = along(up0, {1: 1, 2: 1})
    down1 = along(down0, {1: -1, 2: -1})
    pair1 = across(jnp.where(my_z % 2 == 0, down0, up0))
    up0_p, down0_p, pair0_p = partner(up0), partner(down0), partner(pair0)
    up1, down1, pair1, up0_p, down0_p, pair0_p = tie((up1, down1, pair1, up0_p, down0_p, pair0_p))

    far1 = jnp.where(my_z >= 2, up1, down1)
    up2 = along(jnp.where(my_z == 1, pair0, up1), {1: 1, 2: 1})
    down2 = along(jnp.where(my_z == 2, pair0, down1), {1: -1, 2: -1})
    pair2 = across(far1)
    far1_p, pair1_p = partner(far1), partner(pair1)
    up2, down2, pair2, far1_p, pair1_p = tie((up2, down2, pair2, far1_p, pair1_p))

    far2 = jnp.where(my_z >= 2, up2, down2)
    last_a = across(far2[:half], (0, line - 1))
    last_b = along(pair2[half:], {1: -1, 2: 1})
    far2_p, pair2_p = partner(far2), partner(pair2)
    last_a_p, last_b_p = partner(last_a), partner(last_b)
    held = [own, pair0, up0, down0, far1, pair1, far2, pair2, last_a, last_b]
    held_p = [own_p, pair0_p, up0_p, down0_p, far1_p, pair1_p, far2_p, pair2_p, last_a_p, last_b_p]

    return held + held_p, plan


def shards(queries, latent_cache, block_picks, lengths):
    ctx_count = lax.axis_size("ctx")
    myself = lax.axis_index("ctx")
    owned = latent_cache.shape[0] // BLOCK
    capacity = max(1, 2 * TOPK // ctx_count)
    union_size = 2 * capacity
    own_picks = block_picks[0]
    owners = own_picks // owned
    all_picks = lax.all_to_all(
        jnp.broadcast_to(block_picks, (ctx_count, TOPK)), "ctx", 0, 0, tiled=True
    ).reshape(-1)

    blocks = myself * owned + jnp.arange(owned, dtype=jnp.int32)
    own_flag = jnp.any(all_picks[None, :] == blocks[:, None], axis=1)
    earlier = blocks[None, :] < blocks[:, None]
    rank = jnp.sum((earlier & own_flag[None, :]).astype(jnp.int32), axis=1)
    slot_ids = jnp.arange(union_size, dtype=jnp.int32)
    matches = (rank[None, :] == slot_ids[:, None]) & own_flag[None, :]
    source = jnp.sum(matches.astype(jnp.int32) * jnp.arange(owned, dtype=jnp.int32)[None, :], axis=1)
    own = pack(latent_cache, source)

    named = jnp.zeros((TOPK,), jnp.int32)
    for k in range(owned):
        block = owners * owned + k
        seen = jnp.any(all_picks[None, :] == block[:, None], axis=1) & (block < own_picks)
        named = named + seen.astype(jnp.int32)

    within = jnp.arange(BLOCK, dtype=jnp.int32)
    positions = (own_picks[:, None] * BLOCK + within[None, :]).reshape(1, -1)
    if ctx_count == 16:
        buffers, (buffer_ids, slots, positions) = relay(own, myself, owners, named, positions)
    else:
        buffers = [lax.all_gather(own, "ctx", axis=0, tiled=True)]
        buffer_ids, slots = jnp.zeros_like(owners), owners * union_size + named
    return attend(queries, buffers, buffer_ids, slots, positions, lengths)


def solution(mesh):
    placed = (
        P(("groups", "ctx"), None, None),
        P(("groups", "ctx"), None),
        P(("groups", "ctx"), None),
        P(("groups", "ctx")),
    )
    return jax.shard_map(
        shards,
        mesh=mesh,
        in_specs=placed,
        out_specs=P(("groups", "ctx"), None, None),
        check_vma=False,
    )
```
